32 devices in a mesh: dp: 8 (over y, x, core), mp: 4 (over z).
Axes of the slice: x: 2, y: 2, z: 4, core: 2. Of those that a mesh axis runs over, the one named last changes fastest.
Arguments:
- mel_audio: bfloat16 [32, 80, 2048], P('dp'), may hold values from -6 to 6
- start_noise: bfloat16 [32, 80, 1024], P('dp'), may hold values from -6 to 6
- span_start: int32 [32], replicated, may hold values from 0 to 2047, as said below
- span_length: int32 [32], replicated, may hold values from 1 to 1024, as said below
- block_route: int32 [128], replicated, may hold values from -1 to 47, as said below
- w_input: bfloat16 [160, 1024], replicated, may hold values from -0.5 to 0.5
- attn_gain: float32 [1024], replicated, may hold values from 0.1 to 1.9
- w_qkv: bfloat16 [1024, 3, 1024], P(None, None, 'mp'), may hold values from -4 to 4, as said below
- w_out: bfloat16 [1024, 1024], P('mp'), may hold values from -0.1875 to 0.1875
- final_gain: float32 [1024], replicated, may hold values from 0.1 to 1.9
- w_mel: bfloat16 [80, 1024], replicated, may hold values from -0.1875 to 0.1875
Outputs:
- infilled: float32 [32, 80, 1024], P('dp')
- worker_velocity: float32 [48, 80, 256], P('dp')
The draws below stay inside these ranges and needn't reach their ends.
Inputs may be any that keep to these rules, and one draw needn't show every extreme that they name: Each span lies inside its utterance: span_start[u] + span_length[u] <= 2048. `span_length`: the spans cover 48 blocks of 256 frames in all (the last block of a span may be partly filled). `block_route`: live block slots name worker slots w * 6 + j of worker w, each worker slot exactly once; empty slots hold -1. No worker receives more than 2 blocks from the utterances of one dp index (utterances u with the same u // 4), and some worker receives exactly 2 from one. `w_qkv`: Query, key and value projections in that order along the middle dimension.
All inputs are finite; a program needn't handle non-finite values.
Results may differ from the reference program's by a relative error of at most 0.025.
Values may be sent and summed in bfloat16 or wider, within the bound.
A program may use at most 128 MiB of HBM per device.

```python
import math
import jax
import jax.numpy as jnp
from jax import lax

D = 1024
HEADS = 16
MEL = 80
HEAD_DIM = 64
BLOCK = 256
CTX = 128
BLK_UTT = 4
UTT_DEV = 4
WORK_DEV = 6
EULER = 2
FRAMES = 2048
WIN = 512
SPAN_MAX = 1024
UTTS = 32
SLOTS_ALL = 128
WORK_ALL = 48
N_MP = 4


def span_plan(key):
    split_keys = jax.random.split(jax.random.fold_in(key, 4111), 5)
    spare_blocks = BLK_UTT - 1
    cell_count = UTTS * spare_blocks
    extra_blocks = WORK_ALL - UTTS
    worker_count = WORK_ALL // WORK_DEV
    shuffled = jax.random.permutation(split_keys[0], cell_count)
    cell_rank = jnp.argsort(shuffled, stable=True).astype(jnp.int32)
    chosen = jax.random.randint(split_keys[1], (), 0, UTTS)
    cell_ids = jnp.arange(cell_count, dtype=jnp.int32)
    forced = cell_ids // spare_blocks // UTT_DEV == chosen // UTT_DEV
    cell_score = jnp.where(forced, cell_ids - cell_count, cell_rank)
    placing = jnp.argsort(jnp.argsort(cell_score, stable=True), stable=True)
    taken_mask = (placing < extra_blocks).astype(jnp.int32)
    counts = 1 + jnp.sum(taken_mask.reshape(UTTS, spare_blocks), axis=1)
    remainder = jax.random.randint(split_keys[2], (UTTS,), 1, BLOCK + 1)
    remainder = jnp.where(jnp.arange(UTTS) == chosen, BLOCK, remainder)
    length = (counts - 1) * BLOCK + remainder
    first_frame = jax.random.randint(split_keys[3], (UTTS,), 0, FRAMES - length + 1)
    live_slots = (jnp.arange(BLK_UTT)[None, :] < counts[:, None]).reshape(-1).astype(jnp.int32)
    live_order = jnp.cumsum(live_slots) - live_slots
    workers = jax.random.permutation(split_keys[4], worker_count)
    worker = workers[live_order % worker_count]
    route_table = jnp.where(live_slots > 0, worker * WORK_DEV + live_order // worker_count, -1)
    return (first_frame.astype(jnp.int32), length.astype(jnp.int32), route_table.astype(jnp.int32))


def draw_span_start(key, part):
    return span_plan(key)[0]


def draw_span_length(key, part):
    return span_plan(key)[1]


def draw_block_route(key, part):
    return span_plan(key)[2]


def draw_w_qkv(key, part):
    split_keys = jax.random.split(jax.random.fold_in(key, 977), 1)
    scale = 1.0 / math.sqrt(D)
    drawn = jnp.clip(jax.random.normal(split_keys[0], (D, 3, D)), -6.0, 6.0) * scale
    return drawn.astype(jnp.bfloat16)


def level_of(own_key, shape, pieces, smallest, largest):
    def one(dim, shards_of):
        steps = jax.random.uniform(jax.random.fold_in(jax.random.fold_in(own_key, 6), dim), (shards_of,), jnp.float32, smallest / len(pieces), largest / len(pieces))
        return jnp.repeat(jnp.exp(steps), shape[dim] // shards_of).reshape((-1,) + (1,) * (len(shape) - dim - 1))

    loudness = one(*pieces[0])
    for cut in pieces[1:]:
        loudness = loudness * one(*cut)
    return loudness


def scatter_about(key, extent, scale, limit, cuts=(), held_as=jnp.bfloat16):
    level = level_of(key, extent, cuts, -0.22, 0.18) if cuts else 1.0
    array = jax.random.normal(key, extent, jnp.float32) * scale * level
    return jnp.minimum(jnp.maximum(array, -limit), limit).astype(held_as)


def setup_inputs(seed: int = 0) -> dict:
    arg_keys = jax.random.split(jax.random.key(seed), 12)
    return {
        "mel_audio": scatter_about(arg_keys[0], (UTTS, MEL, FRAMES), 1.0, 6.0, ((0, 8),)),
        "start_noise": scatter_about(arg_keys[1], (UTTS, MEL, SPAN_MAX), 1.0, 6.0, ((0, 8),)),
        "span_start": draw_span_start(jax.random.fold_in(arg_keys[11], 71), 0),
        "span_length": draw_span_length(jax.random.fold_in(arg_keys[11], 71), 0),
        "block_route": draw_block_route(jax.random.fold_in(arg_keys[11], 71), 0),
        "w_input": scatter_about(arg_keys[5], (2 * MEL, D), (2 * MEL) ** -0.5, 0.5),
        "attn_gain": jnp.clip(1.0 + 0.18 * jax.random.normal(arg_keys[6], (D,), jnp.float32), 0.1, 1.9),
        "w_qkv": draw_w_qkv(jax.random.fold_in(arg_keys[11], 71), 0),
        "w_out": scatter_about(arg_keys[8], (D, D), D ** -0.5, 0.1875, ((0, 4),)),
        "final_gain": jnp.clip(1.0 + 0.18 * jax.random.normal(arg_keys[9], (D,), jnp.float32), 0.1, 1.9),
        "w_mel": scatter_about(arg_keys[10], (MEL, D), D ** -0.5, 0.1875),
    }


flow_steps = 32.0
norm_eps = 1e-05

def time_embed(t_value, feature_width):
    half_width = feature_width // 2
    freqs = jnp.exp(-math.log(10000.0) * jnp.arange(half_width, dtype=jnp.float32) / half_width)
    angles = 1000.0 * t_value * freqs
    return jnp.concatenate([jnp.sin(angles), jnp.cos(angles)])

def layer_norm(hidden, norm_gain):
    mean_value = lax.optimization_barrier(jnp.mean(hidden, axis=-1, keepdims=True))
    centred = hidden - mean_value
    variance = lax.optimization_barrier(jnp.mean(centred * centred, axis=-1, keepdims=True))
    return centred * lax.rsqrt(variance + norm_eps) * norm_gain.astype(jnp.float32)

def velocity(window, window_begin, own_count, t_value, w_input, attn_gain, w_qkv, w_out, final_gain, w_mel):
    hidden = jnp.dot(window.T, w_input, preferred_element_type=jnp.float32)
    hidden = hidden + time_embed(t_value, D)[None, :]
    normed = layer_norm(hidden, attn_gain).astype(jnp.bfloat16)
    queries = jnp.dot(normed[CTX:CTX + BLOCK], w_qkv[:, 0, :], preferred_element_type=jnp.float32).astype(jnp.bfloat16)
    key_rows = jnp.dot(normed, w_qkv[:, 1, :], preferred_element_type=jnp.float32).astype(jnp.bfloat16)
    value_rows = jnp.dot(normed, w_qkv[:, 2, :], preferred_element_type=jnp.float32).astype(jnp.bfloat16)
    query_heads = queries.astype(jnp.float32).reshape(BLOCK, HEADS, HEAD_DIM)
    key_heads = key_rows.astype(jnp.float32).reshape(WIN, HEADS, HEAD_DIM)
    value_heads = value_rows.astype(jnp.float32).reshape(WIN, HEADS, HEAD_DIM)
    scores = jnp.einsum('qhd,khd->hqk', query_heads, key_heads) * (1.0 / math.sqrt(HEAD_DIM))
    position = window_begin - CTX + jnp.arange(WIN, dtype=jnp.int32)
    usable = (position >= 0) & (position < FRAMES)
    scores = jnp.where(usable[None, None, :], scores, -1e+30)
    attn_weights = jax.nn.softmax(scores, axis=-1).astype(jnp.bfloat16)
    head_outputs = jnp.einsum('hqk,khd->qhd', attn_weights.astype(jnp.float32), value_heads)
    head_outputs = head_outputs.astype(jnp.bfloat16).reshape(BLOCK, D)
    group_width = D // N_MP
    attended = jnp.zeros((BLOCK, D), jnp.float32)
    for mp_part in range(N_MP):
        lower = mp_part * group_width
        term = jnp.dot(head_outputs[:, lower:lower + group_width], w_out[lower:lower + group_width], preferred_element_type=jnp.float32)
        attended = attended + term.astype(jnp.bfloat16).astype(jnp.float32)
    final = layer_norm(hidden[CTX:CTX + BLOCK] + attended, final_gain).astype(jnp.bfloat16)
    result = jnp.dot(w_mel, final.T, preferred_element_type=jnp.float32)
    live_mask = jnp.arange(BLOCK, dtype=jnp.int32) < own_count
    return jnp.where(live_mask[None, :], result, 0.0)

def reference(mel_audio, start_noise, span_start, span_length, block_route, w_input, attn_gain, w_qkv, w_out, final_gain, w_mel):
    slot_ids = jnp.arange(WORK_ALL, dtype=jnp.int32)
    every_slot = jnp.arange(SLOTS_ALL, dtype=jnp.int32)
    matches = block_route[None, :] == slot_ids[:, None]
    blocks = lax.optimization_barrier(jnp.sum(jnp.where(matches, every_slot[None, :], 0), axis=1)).astype(jnp.int32)
    padded = jnp.pad(mel_audio, ((0, 0), (0, 0), (CTX, SPAN_MAX + CTX)))
    zero_index = jnp.zeros((), jnp.int32)

    def solve_block(block_index):
        utterance = (block_index // BLK_UTT).astype(jnp.int32)
        block_order = (block_index % BLK_UTT).astype(jnp.int32)
        first_frame = span_start[utterance]
        length = span_length[utterance]
        window_begin = (first_frame + BLOCK * block_order).astype(jnp.int32)
        audio_rows = lax.dynamic_slice(padded, (utterance, zero_index, window_begin), (1, MEL, WIN))[0]
        position = window_begin - CTX + jnp.arange(WIN, dtype=jnp.int32)
        in_span = (position >= first_frame) & (position < first_frame + length)
        context = jnp.where(in_span[None, :], jnp.zeros((), jnp.bfloat16), audio_rows)
        own_count = jnp.minimum(BLOCK, length - BLOCK * block_order)
        live_mask = jnp.arange(BLOCK, dtype=jnp.int32) < own_count
        frames_state = lax.dynamic_slice(start_noise, (utterance, zero_index, (BLOCK * block_order).astype(jnp.int32)), (1, MEL, BLOCK))[0].astype(jnp.float32)
        side_zeros = jnp.zeros((MEL, CTX), jnp.bfloat16)
        result = jnp.zeros((MEL, BLOCK), jnp.float32)
        total = jnp.zeros((MEL, BLOCK), jnp.float32)
        for euler_step in range(EULER):
            state_rows = jnp.where(live_mask[None, :], frames_state, 0.0).astype(jnp.bfloat16)
            state_window = jnp.concatenate([side_zeros, state_rows, side_zeros], axis=1)
            window = jnp.concatenate([context, state_window], axis=0)
            result = velocity(window, window_begin, own_count, euler_step / flow_steps, w_input, attn_gain, w_qkv, w_out, final_gain, w_mel)
            frames_state = frames_state + result * (1.0 / flow_steps)
            total = total + result
        return (result, jnp.where(live_mask[None, :], total, 0.0))
    worker_velocity, finals = lax.map(solve_block, blocks)
    slotted = jnp.zeros((SLOTS_ALL, MEL, BLOCK), jnp.float32).at[blocks].set(finals)
    infilled = slotted.reshape(UTTS, BLK_UTT, MEL, BLOCK).transpose(0, 2, 1, 3).reshape(UTTS, MEL, SPAN_MAX)
    return (infilled, worker_velocity)
```

```python
import math

import jax
import jax.numpy as jnp
from jax import lax
from jax.sharding import PartitionSpec as P

MEL = 80
HEAD_DIM = 64
BLOCK = 256
CTX = 128
BLK_UTT = 4
UTT_DEV = 4
WORK_DEV = 6
EULER = 2
FRAMES = 2048
WIN = 512
SPAN_MAX = 1024
SLOT_DEV = 16


flow_steps = 32.0
norm_eps = 1e-05


def time_embed(t_value, feature_width):
    half_width = feature_width // 2
    freqs = jnp.exp(-math.log(10000.0) * jnp.arange(half_width, dtype=jnp.float32) / half_width)
    angles = 1000.0 * t_value * freqs
    return jnp.concatenate([jnp.sin(angles), jnp.cos(angles)])


def layer_norm(hidden, norm_gain):
    mean_value = jnp.mean(hidden, axis=-1, keepdims=True)
    centred = hidden - mean_value
    variance = jnp.mean(centred * centred, axis=-1, keepdims=True)
    return centred * lax.rsqrt(variance + norm_eps) * norm_gain


def owner_windows(mel_part, noise_part, first_frames, lengths):
    channels = mel_part.shape[1]
    reach = SPAN_MAX + 2 * CTX
    padded = jnp.pad(mel_part, ((0, 0), (0, 0), (CTX, SPAN_MAX + CTX)))
    regions = jnp.stack(
        [lax.dynamic_slice_in_dim(padded[u], first_frames[u], reach, 1) for u in range(UTT_DEV)]
    )
    offsets = jnp.arange(reach, dtype=jnp.int32)[None, :] - CTX
    in_span = (offsets >= 0) & (offsets < lengths[:, None])
    regions = jnp.where(in_span[:, None, :], jnp.zeros((), jnp.bfloat16), regions)
    live_mask = jnp.arange(SPAN_MAX, dtype=jnp.int32)[None, :] < lengths[:, None]
    current = jnp.where(live_mask[:, None, :], noise_part, jnp.zeros((), jnp.bfloat16))
    blocks = [
        jnp.concatenate(
            [
                regions[:, :, BLOCK * k : BLOCK * k + WIN],
                current[:, :, BLOCK * k : BLOCK * (k + 1)],
            ],
            axis=2,
        )
        for k in range(BLK_UTT)
    ]
    return jnp.stack(blocks, axis=1).reshape(SLOT_DEV, channels, WIN + BLOCK)


def owner_targets(block_route, dp_count, capacity):
    owner_index = lax.axis_index("dp")
    destination = lax.dynamic_slice_in_dim(block_route, owner_index * SLOT_DEV, SLOT_DEV, 0)
    live = destination >= 0
    worker = jnp.where(live, destination // WORK_DEV, -1)
    earlier = (
        (worker[:, None] == worker[None, :])
        & (destination[None, :] < destination[:, None])
        & live[None, :]
    )
    rank = jnp.sum(earlier.astype(jnp.int32), axis=1)
    position = worker * capacity + rank
    rows = jnp.arange(dp_count * capacity, dtype=jnp.int32)
    return (rows[:, None] == position[None, :]) & live[None, :]


def worker_plan(block_route, span_start, span_length, dp_count, capacity):
    worker_index = lax.axis_index("dp")
    slot_ids = worker_index * WORK_DEV + jnp.arange(WORK_DEV, dtype=jnp.int32)
    every_slot = jnp.arange(block_route.shape[0], dtype=jnp.int32)
    matches = block_route[None, :] == slot_ids[:, None]
    block_index = jnp.sum(jnp.where(matches, every_slot[None, :], 0), axis=1)
    owner = block_index // SLOT_DEV
    utterance = block_index // BLK_UTT
    block_order = block_index % BLK_UTT
    utter_ids = jnp.arange(span_start.shape[0], dtype=jnp.int32)
    pick_utter = utterance[:, None] == utter_ids[None, :]
    first_frame = jnp.sum(jnp.where(pick_utter, span_start[None, :], 0), axis=1)
    length = jnp.sum(jnp.where(pick_utter, span_length[None, :], 0), axis=1)
    window_begin = first_frame + BLOCK * block_order
    own_count = jnp.minimum(BLOCK, length - BLOCK * block_order)
    local_ids = jnp.arange(WORK_DEV, dtype=jnp.int32)
    earlier = (owner[:, None] == owner[None, :]) & (local_ids[None, :] < local_ids[:, None])
    rank = jnp.sum(earlier.astype(jnp.int32), axis=1)
    position = owner * capacity + rank
    pick_owner = position[:, None] == jnp.arange(dp_count * capacity, dtype=jnp.int32)[None, :]
    return (pick_owner, window_begin, own_count)


def attend(queries, key_rows, value_rows, usable):
    head_count = queries.shape[1] // HEAD_DIM
    query_heads = queries.reshape(queries.shape[0], head_count, HEAD_DIM)
    key_heads = key_rows.reshape(WIN, head_count, HEAD_DIM)
    value_heads = value_rows.reshape(WIN, head_count, HEAD_DIM)
    scores = jnp.einsum(
        "qhd,khd->hqk", query_heads, key_heads, preferred_element_type=jnp.float32
    ) * (1.0 / math.sqrt(HEAD_DIM))
    scores = jnp.where(usable[None, None, :], scores, -1e30)
    attn_weights = jax.nn.softmax(scores, axis=-1).astype(jnp.bfloat16)
    head_outputs = jnp.einsum(
        "hqk,khd->qhd", attn_weights, value_heads, preferred_element_type=jnp.float32
    )
    return head_outputs.astype(jnp.bfloat16).reshape(queries.shape)


def block_velocity(window, usable, first_row, row_count, t_value, weights):
    w_input, attn_gain, w_q, w_k, w_v, w_out_t, final_gain, w_mel = weights
    hidden = jnp.einsum("scf,cd->sfd", window, w_input, preferred_element_type=jnp.float32)
    hidden = hidden + time_embed(t_value, w_input.shape[1])[None, None, :]
    normed = layer_norm(hidden, attn_gain).astype(jnp.bfloat16)

    def own_rows(rows):
        second = lax.dynamic_slice_in_dim(rows[1], CTX + first_row, row_count, 0)
        return jnp.concatenate([rows[0, CTX : CTX + BLOCK], second], axis=0)

    def project(rows, weight):
        return jnp.dot(rows, weight, preferred_element_type=jnp.float32).astype(jnp.bfloat16)

    queries = project(own_rows(normed), w_q)
    flat = normed.reshape(2 * WIN, normed.shape[2])
    key_rows = project(flat, w_k)
    value_rows = project(flat, w_v)
    head_outputs = jnp.concatenate(
        [
            attend(queries[:BLOCK], key_rows[:WIN], value_rows[:WIN], usable[0]),
            attend(queries[BLOCK:], key_rows[WIN:], value_rows[WIN:], usable[1]),
        ],
        axis=0,
    )
    attended = jnp.einsum(
        "qe,de->qd", head_outputs, w_out_t, preferred_element_type=jnp.float32
    )
    final = layer_norm(own_rows(hidden) + attended, final_gain).astype(jnp.bfloat16)
    return jnp.einsum("md,qd->mq", w_mel, final, preferred_element_type=jnp.float32)


def gather_weights(w_qkv, w_out):
    dp_count = lax.axis_size("dp")
    mp_count = lax.axis_size("mp")
    dp_index = lax.axis_index("dp")
    depth, columns = w_qkv.shape[0], w_qkv.shape[2]
    rows = depth // dp_count
    part = lax.dynamic_slice_in_dim(w_qkv, dp_index * rows, rows, 0).transpose(1, 0, 2)
    out_part = lax.dynamic_slice_in_dim(w_out, dp_index * rows, rows, 1).T
    mine = jnp.concatenate([part, out_part[None]], axis=0)
    gathered = lax.all_gather(mine, ("dp", "mp"), axis=0, tiled=False)
    gathered = gathered.reshape(dp_count, mp_count, 4, rows, columns)
    return [
        gathered[:, :, i].transpose(0, 2, 1, 3).reshape(depth, mp_count * columns)
        for i in range(4)
    ]


def to_span(slot_values):
    return (
        slot_values.reshape(UTT_DEV, BLK_UTT, MEL, BLOCK)
        .transpose(0, 2, 1, 3)
        .reshape(UTT_DEV, MEL, SPAN_MAX)
    )


def shards(
    mel_audio,
    start_noise,
    span_start,
    span_length,
    block_route,
    w_input,
    attn_gain,
    w_qkv,
    w_out,
    final_gain,
    w_mel,
):
    dp_count = lax.axis_size("dp")
    capacity = (SLOT_DEV + dp_count - 1) // dp_count
    owner_index = lax.axis_index("dp")
    first_frames = lax.dynamic_slice_in_dim(span_start, owner_index * UTT_DEV, UTT_DEV, 0)
    lengths = lax.dynamic_slice_in_dim(span_length, owner_index * UTT_DEV, UTT_DEV, 0)
    targets = owner_targets(block_route, dp_count, capacity)
    target_rows = targets.astype(jnp.bfloat16)
    pick_owner, window_begin, own_count = worker_plan(
        block_route, span_start, span_length, dp_count, capacity
    )
    w_q, w_k, w_v, w_out_t = gather_weights(w_qkv, w_out)
    weights = (w_input, attn_gain, w_q, w_k, w_v, w_out_t, final_gain, w_mel)
    mp_count = lax.axis_size("mp")
    mp_index = lax.axis_index("mp")
    group = 2 * WORK_DEV // mp_count
    channels = MEL // mp_count
    mel_part = lax.dynamic_slice_in_dim(mel_audio, mp_index * channels, channels, 1)
    noise_part = lax.dynamic_slice_in_dim(start_noise, mp_index * channels, channels, 1)
    windows = owner_windows(mel_part, noise_part, first_frames, lengths)
    outgoing = jnp.einsum(
        "ws,scf->wcf", target_rows, windows, preferred_element_type=jnp.float32
    ).astype(jnp.bfloat16)
    received = lax.all_to_all(outgoing, "dp", split_axis=0, concat_axis=0, tiled=True)
    pairs = []
    for m in range(mp_count):
        pairs += [group * (m // 2) + (group - 1) * (m % 2), group * (m // 2) + 1]
    pick_pairs = jnp.concatenate([pick_owner[j : j + 1] for j in pairs], axis=0)
    spread = jnp.einsum(
        "so,ocf->scf",
        pick_pairs.astype(jnp.bfloat16),
        received,
        preferred_element_type=jnp.float32,
    ).astype(jnp.bfloat16)
    mine = lax.all_to_all(spread, "mp", split_axis=0, concat_axis=0, tiled=True)
    mine = mine.reshape(mp_count, 2, channels, WIN + BLOCK).transpose(1, 0, 2, 3)
    mine = mine.reshape(2, MEL, WIN + BLOCK)
    pair_begin = lax.dynamic_slice_in_dim(
        jnp.stack([window_begin[j] for j in pairs]), 2 * mp_index, 2, 0
    )
    pair_count = lax.dynamic_slice_in_dim(
        jnp.stack([own_count[j] for j in pairs]), 2 * mp_index, 2, 0
    )
    position = pair_begin[:, None] - CTX + jnp.arange(WIN, dtype=jnp.int32)[None, :]
    usable = (position >= 0) & (position < FRAMES)
    columns = jnp.arange(BLOCK, dtype=jnp.int32)
    live_mask = columns[None, :] < pair_count[:, None]
    half = BLOCK // 2
    first_row = (mp_index % 2) * half
    context = mine[:, :, :WIN]
    block_state = mine[:, :, WIN:].astype(jnp.float32)
    half_total = jnp.zeros((MEL, BLOCK + half), jnp.float32)
    for euler_step in range(EULER):
        state_rows = jnp.where(live_mask[:, None, :], block_state, 0.0).astype(jnp.bfloat16)
        state_window = jnp.pad(state_rows, ((0, 0), (0, 0), (CTX, CTX)))
        window = jnp.concatenate([context, state_window], axis=1)
        last = euler_step == EULER - 1
        row_begin, row_count = (first_row, half) if last else (0, BLOCK)
        result = block_velocity(
            window, usable, row_begin, row_count, euler_step / flow_steps, weights
        )
        if last:
            own_live = jnp.concatenate(
                [live_mask[0], lax.dynamic_slice_in_dim(live_mask[1], first_row, half, 0)]
            )
            velocity = jnp.where(own_live[None, :], result, 0.0)
            half_total = half_total + velocity
        else:
            both = jnp.stack([result[:, :BLOCK], result[:, BLOCK:]])
            both = jnp.where(live_mask[:, None, :], both, 0.0)
            block_state = block_state + both * (1.0 / flow_steps)
            own = lax.dynamic_slice_in_dim(both[1], first_row, half, 1)
            half_total = half_total + jnp.concatenate([both[0], own], axis=1)

    def whole_blocks(halves):
        blocks = []
        for pair in range(mp_count // 2):
            one, other = halves[2 * pair], halves[2 * pair + 1]
            middle = jnp.concatenate([one[:, BLOCK:], other[:, BLOCK:]], axis=1)
            blocks += [one[:, :BLOCK], middle, other[:, :BLOCK]]
        return jnp.stack(blocks)

    finals = whole_blocks(lax.all_gather(half_total.astype(jnp.bfloat16), "mp"))
    result = whole_blocks(lax.all_gather(velocity, "mp"))
    returned = jnp.einsum(
        "so,smq->omq",
        pick_owner.astype(jnp.bfloat16),
        finals,
        preferred_element_type=jnp.float32,
    )
    arrived = lax.all_to_all(
        returned.astype(jnp.bfloat16), "dp", split_axis=0, concat_axis=0, tiled=True
    )
    slot_values = jnp.einsum(
        "ws,wmq->smq", target_rows, arrived, preferred_element_type=jnp.float32
    )
    infilled = to_span(slot_values)
    return (infilled, result)


def solution(mesh):
    return jax.shard_map(
        shards,
        mesh=mesh,
        in_specs=(
            P("dp", None, None),
            P("dp", None, None),
            P(),
            P(),
            P(),
            P(),
            P(),
            P(None, None, "mp"),
            P("mp", None),
            P(),
            P(),
        ),
        out_specs=(P("dp", None, None), P("dp", None, None)),
        check_vma=False,
    )
```

```python
import math

import jax
import jax.numpy as jnp
from jax import lax
from jax.experimental import pallas as pl
from jax.experimental.pallas import tpu as pltpu
from jax.sharding import PartitionSpec as P

MEL = 80
HEAD_DIM = 64
BLOCK = 256
CTX = 128
BLK_UTT = 4
UTT_DEV = 4
WORK_DEV = 6
EULER = 2
FRAMES = 2048
WIN = 512
SPAN_MAX = 1024
SLOT_DEV = 16


flow_steps = 32.0
norm_eps = 1e-05


def time_embed(t_value, feature_width):
    half_width = feature_width // 2
    freqs = jnp.exp(-math.log(10000.0) * jnp.arange(half_width, dtype=jnp.float32) / half_width)
    angles = 1000.0 * t_value * freqs
    return jnp.concatenate([jnp.sin(angles), jnp.cos(angles)])


def layer_norm(hidden, norm_gain):
    mean_value = jnp.mean(hidden, axis=-1, keepdims=True)
    centred = hidden - mean_value
    variance = jnp.mean(centred * centred, axis=-1, keepdims=True)
    return centred * lax.rsqrt(variance + norm_eps) * norm_gain


def owner_windows(mel_part, noise_part, first_frames, lengths):
    channels = mel_part.shape[1]
    reach = SPAN_MAX + 2 * CTX
    padded = jnp.pad(mel_part, ((0, 0), (0, 0), (CTX, SPAN_MAX + CTX)))
    regions = jnp.stack(
        [lax.dynamic_slice_in_dim(padded[u], first_frames[u], reach, 1) for u in range(UTT_DEV)]
    )
    offsets = jnp.arange(reach, dtype=jnp.int32)[None, :] - CTX
    in_span = (offsets >= 0) & (offsets < lengths[:, None])
    regions = jnp.where(in_span[:, None, :], jnp.zeros((), jnp.bfloat16), regions)
    live_mask = jnp.arange(SPAN_MAX, dtype=jnp.int32)[None, :] < lengths[:, None]
    current = jnp.where(live_mask[:, None, :], noise_part, jnp.zeros((), jnp.bfloat16))
    blocks = [
        jnp.concatenate(
            [
                regions[:, :, BLOCK * k : BLOCK * k + WIN],
                current[:, :, BLOCK * k : BLOCK * (k + 1)],
            ],
            axis=2,
        )
        for k in range(BLK_UTT)
    ]
    return jnp.stack(blocks, axis=1).reshape(SLOT_DEV, channels, WIN + BLOCK)


def owner_targets(block_route, dp_count, capacity):
    owner_index = lax.axis_index("dp")
    destination = lax.dynamic_slice_in_dim(block_route, owner_index * SLOT_DEV, SLOT_DEV, 0)
    live = destination >= 0
    worker = jnp.where(live, destination // WORK_DEV, -1)
    earlier = (
        (worker[:, None] == worker[None, :])
        & (destination[None, :] < destination[:, None])
        & live[None, :]
    )
    rank = jnp.sum(earlier.astype(jnp.int32), axis=1)
    position = worker * capacity + rank
    rows = jnp.arange(dp_count * capacity, dtype=jnp.int32)
    return (rows[:, None] == position[None, :]) & live[None, :]


def worker_plan(block_route, span_start, span_length, dp_count, capacity):
    worker_index = lax.axis_index("dp")
    slot_ids = worker_index * WORK_DEV + jnp.arange(WORK_DEV, dtype=jnp.int32)
    every_slot = jnp.arange(block_route.shape[0], dtype=jnp.int32)
    matches = block_route[None, :] == slot_ids[:, None]
    block_index = jnp.sum(jnp.where(matches, every_slot[None, :], 0), axis=1)
    owner = block_index // SLOT_DEV
    utterance = block_index // BLK_UTT
    block_order = block_index % BLK_UTT
    utter_ids = jnp.arange(span_start.shape[0], dtype=jnp.int32)
    pick_utter = utterance[:, None] == utter_ids[None, :]
    first_frame = jnp.sum(jnp.where(pick_utter, span_start[None, :], 0), axis=1)
    length = jnp.sum(jnp.where(pick_utter, span_length[None, :], 0), axis=1)
    window_begin = first_frame + BLOCK * block_order
    own_count = jnp.minimum(BLOCK, length - BLOCK * block_order)
    local_ids = jnp.arange(WORK_DEV, dtype=jnp.int32)
    earlier = (owner[:, None] == owner[None, :]) & (local_ids[None, :] < local_ids[:, None])
    rank = jnp.sum(earlier.astype(jnp.int32), axis=1)
    position = owner * capacity + rank
    pick_owner = position[:, None] == jnp.arange(dp_count * capacity, dtype=jnp.int32)[None, :]
    return (pick_owner, window_begin, own_count)


def attention_kernel(own_ref, rows_ref, usable_ref, w_q_ref, w_k_ref, w_v_ref, out_ref):
    def project(rows, weight_ref):
        return jnp.dot(
            rows[...], weight_ref[0], preferred_element_type=jnp.float32
        ).astype(jnp.bfloat16)

    queries = project(own_ref, w_q_ref)
    key_rows = project(rows_ref, w_k_ref)
    value_rows = project(rows_ref, w_v_ref)
    width = queries.shape[1]
    head_of_lane = lax.broadcasted_iota(jnp.int32, (1, width), 1) // HEAD_DIM
    for block, (begin, end) in enumerate(((0, BLOCK), (BLOCK, own_ref.shape[0]))):
        block_queries = queries[begin:end]
        block_keys = key_rows[block * WIN : (block + 1) * WIN]
        block_values = value_rows[block * WIN : (block + 1) * WIN]
        usable = usable_ref[block : block + 1, :] > 0
        collected = jnp.zeros((end - begin, width), jnp.float32)
        for head in range(width // HEAD_DIM):
            mine = head_of_lane == head
            head_queries = jnp.where(mine, block_queries, jnp.zeros((), jnp.bfloat16))
            scores = lax.dot_general(
                head_queries,
                block_keys,
                (((1,), (1,)), ((), ())),
                preferred_element_type=jnp.float32,
            )
            scores = jnp.where(usable, scores * (1.0 / math.sqrt(HEAD_DIM)), -1e30)
            weights = jnp.exp(scores - jnp.max(scores, axis=1, keepdims=True))
            norm = jnp.sum(weights, axis=1, keepdims=True)
            product = jnp.dot(
                weights.astype(jnp.bfloat16), block_values, preferred_element_type=jnp.float32
            )
            collected = jnp.where(mine, product * (1.0 / norm), collected)
        out_ref[begin:end, :] = collected.astype(jnp.bfloat16)


def attention(own, rows, usable, w_q, w_k, w_v):
    groups, depth, columns = w_q.shape
    count = own.shape[0]
    weight_spec = pl.BlockSpec((1, depth, columns), lambda g: (g, 0, 0))
    return pl.pallas_call(
        attention_kernel,
        grid=(groups,),
        out_shape=jax.ShapeDtypeStruct((count, groups * columns), jnp.bfloat16),
        in_specs=[
            pl.BlockSpec((count, depth), lambda g: (0, 0)),
            pl.BlockSpec(rows.shape, lambda g: (0, 0)),
            pl.BlockSpec(usable.shape, lambda g: (0, 0)),
            weight_spec,
            weight_spec,
            weight_spec,
        ],
        out_specs=pl.BlockSpec((count, columns), lambda g: (0, g)),
        cost_estimate=pl.CostEstimate(
            flops=2 * groups * columns * depth * (count + 2 * rows.shape[0]) * 2,
            bytes_accessed=3 * groups * depth * columns * 2,
            transcendentals=count * WIN * groups * columns // HEAD_DIM,
        ),
        compiler_params=pltpu.CompilerParams(vmem_limit_bytes=40 * 1024 * 1024),
    )(own, rows, usable, w_q, w_k, w_v)


def block_velocity(window, usable, first_row, row_count, t_value, weights):
    w_input, attn_gain, w_q, w_k, w_v, w_out, final_gain, w_mel = weights
    hidden = jnp.einsum("scf,cd->sfd", window, w_input, preferred_element_type=jnp.float32)
    hidden = hidden + time_embed(t_value, w_input.shape[1])[None, None, :]
    normed = layer_norm(hidden, attn_gain).astype(jnp.bfloat16)

    def own_rows(rows):
        second = lax.dynamic_slice_in_dim(rows[1], CTX + first_row, row_count, 0)
        return jnp.concatenate([rows[0, CTX : CTX + BLOCK], second], axis=0)

    head_outputs = attention(
        own_rows(normed), normed.reshape(2 * WIN, normed.shape[2]), usable, w_q, w_k, w_v
    )
    attended = jnp.dot(head_outputs, w_out, preferred_element_type=jnp.float32)
    final = layer_norm(own_rows(hidden) + attended, final_gain).astype(jnp.bfloat16)
    return jnp.einsum("md,qd->mq", w_mel, final, preferred_element_type=jnp.float32)


def gather_weights(w_qkv, w_out):
    dp_count = lax.axis_size("dp")
    mp_count = lax.axis_size("mp")
    dp_index = lax.axis_index("dp")
    depth, columns = w_qkv.shape[0], w_qkv.shape[2]
    rows = depth // dp_count
    part = lax.dynamic_slice_in_dim(w_qkv, dp_index * rows, rows, 0)
    gathered = []
    for i in range(3):
        whole = lax.all_gather(part[:, i, :], ("mp", "dp"), axis=0, tiled=True)
        gathered.append(whole.reshape(mp_count, depth, columns))
    out_rows = w_out.shape[0] // dp_count
    out_part = lax.dynamic_slice_in_dim(w_out, dp_index * out_rows, out_rows, 0)
    gathered.append(lax.all_gather(out_part, ("mp", "dp"), axis=0, tiled=True))
    return gathered


def to_span(slot_values):
    return (
        slot_values.reshape(UTT_DEV, BLK_UTT, MEL, BLOCK)
        .transpose(0, 2, 1, 3)
        .reshape(UTT_DEV, MEL, SPAN_MAX)
    )


def shards(
    mel_audio,
    start_noise,
    span_start,
    span_length,
    block_route,
    w_input,
    attn_gain,
    w_qkv,
    w_out,
    final_gain,
    w_mel,
):
    dp_count = lax.axis_size("dp")
    capacity = (SLOT_DEV + dp_count - 1) // dp_count
    owner_index = lax.axis_index("dp")
    first_frames = lax.dynamic_slice_in_dim(span_start, owner_index * UTT_DEV, UTT_DEV, 0)
    lengths = lax.dynamic_slice_in_dim(span_length, owner_index * UTT_DEV, UTT_DEV, 0)
    targets = owner_targets(block_route, dp_count, capacity)
    target_rows = targets.astype(jnp.bfloat16)
    pick_owner, window_begin, own_count = worker_plan(
        block_route, span_start, span_length, dp_count, capacity
    )
    w_q, w_k, w_v, w_out_all = gather_weights(w_qkv, w_out)
    weights = (w_input, attn_gain, w_q, w_k, w_v, w_out_all, final_gain, w_mel)
    mp_count = lax.axis_size("mp")
    mp_index = lax.axis_index("mp")
    group = 2 * WORK_DEV // mp_count
    channels = MEL // mp_count
    mel_part = lax.dynamic_slice_in_dim(mel_audio, mp_index * channels, channels, 1)
    noise_part = lax.dynamic_slice_in_dim(start_noise, mp_index * channels, channels, 1)
    windows = owner_windows(mel_part, noise_part, first_frames, lengths)
    outgoing = jnp.einsum(
        "ws,scf->wcf", target_rows, windows, preferred_element_type=jnp.float32
    ).astype(jnp.bfloat16)
    received = lax.all_to_all(outgoing, "dp", split_axis=0, concat_axis=0, tiled=True)
    pairs = []
    for m in range(mp_count):
        pairs += [group * (m // 2) + (group - 1) * (m % 2), group * (m // 2) + 1]
    pick_pairs = jnp.concatenate([pick_owner[j : j + 1] for j in pairs], axis=0)
    spread = jnp.einsum(
        "so,ocf->scf",
        pick_pairs.astype(jnp.bfloat16),
        received,
        preferred_element_type=jnp.float32,
    ).astype(jnp.bfloat16)
    mine = lax.all_to_all(spread, "mp", split_axis=0, concat_axis=0, tiled=True)
    mine = mine.reshape(mp_count, 2, channels, WIN + BLOCK).transpose(1, 0, 2, 3)
    mine = mine.reshape(2, MEL, WIN + BLOCK)
    pair_begin = lax.dynamic_slice_in_dim(
        jnp.stack([window_begin[j] for j in pairs]), 2 * mp_index, 2, 0
    )
    pair_count = lax.dynamic_slice_in_dim(
        jnp.stack([own_count[j] for j in pairs]), 2 * mp_index, 2, 0
    )
    position = pair_begin[:, None] - CTX + jnp.arange(WIN, dtype=jnp.int32)[None, :]
    usable = ((position >= 0) & (position < FRAMES)).astype(jnp.int32)
    columns = jnp.arange(BLOCK, dtype=jnp.int32)
    live_mask = columns[None, :] < pair_count[:, None]
    half = BLOCK // 2
    first_row = (mp_index % 2) * half
    context = mine[:, :, :WIN]
    block_state = mine[:, :, WIN:].astype(jnp.float32)
    half_total = jnp.zeros((MEL, BLOCK + half), jnp.float32)
    for euler_step in range(EULER):
        state_rows = jnp.where(live_mask[:, None, :], block_state, 0.0).astype(jnp.bfloat16)
        state_window = jnp.pad(state_rows, ((0, 0), (0, 0), (CTX, CTX)))
        window = jnp.concatenate([context, state_window], axis=1)
        last = euler_step == EULER - 1
        row_begin, row_count = (first_row, half) if last else (0, BLOCK)
        result = block_velocity(
            window, usable, row_begin, row_count, euler_step / flow_steps, weights
        )
        if last:
            own_live = jnp.concatenate(
                [live_mask[0], lax.dynamic_slice_in_dim(live_mask[1], first_row, half, 0)]
            )
            velocity = jnp.where(own_live[None, :], result, 0.0)
            half_total = half_total + velocity
        else:
            both = jnp.stack([result[:, :BLOCK], result[:, BLOCK:]])
            both = jnp.where(live_mask[:, None, :], both, 0.0)
            block_state = block_state + both * (1.0 / flow_steps)
            own = lax.dynamic_slice_in_dim(both[1], first_row, half, 1)
            half_total = half_total + jnp.concatenate([both[0], own], axis=1)

    def whole_blocks(halves):
        blocks = []
        for pair in range(mp_count // 2):
            one, other = halves[2 * pair], halves[2 * pair + 1]
            middle = jnp.concatenate([one[:, BLOCK:], other[:, BLOCK:]], axis=1)
            blocks += [one[:, :BLOCK], middle, other[:, :BLOCK]]
        return jnp.stack(blocks)

    both = jnp.concatenate([half_total, velocity], axis=1).astype(jnp.bfloat16)
    both = lax.all_gather(both, "mp")
    finals = whole_blocks(both[:, :, : BLOCK + half])
    result = whole_blocks(both[:, :, BLOCK + half :]).astype(jnp.float32)
    returned = jnp.einsum(
        "so,smq->omq",
        pick_owner.astype(jnp.bfloat16),
        finals,
        preferred_element_type=jnp.float32,
    )
    arrived = lax.all_to_all(
        returned.astype(jnp.bfloat16), "dp", split_axis=0, concat_axis=0, tiled=True
    )
    slot_values = jnp.einsum(
        "ws,wmq->smq", target_rows, arrived, preferred_element_type=jnp.float32
    )
    infilled = to_span(slot_values)
    return (infilled, result)


def solution(mesh):
    return jax.shard_map(
        shards,
        mesh=mesh,
        in_specs=(
            P("dp", None, None),
            P("dp", None, None),
            P(),
            P(),
            P(),
            P(),
            P(),
            P(None, None, "mp"),
            P("mp", None),
            P(),
            P(),
        ),
        out_specs=(P("dp", None, None), P("dp", None, None)),
        check_vma=False,
    )
```
